32 devices in a mesh: section: 4 (over y, x), dp: 8 (over z, core).
Axes of the slice: x: 2, y: 2, z: 4, core: 2. Of those that a mesh axis runs over, the one named last changes fastest.
Arguments:
- inputs: bfloat16 [4, 2, 512, 4096], P('section', None, 'dp'), may hold values from -6 to 6
- cotangent: bfloat16 [2, 512, 4096], P(None, 'dp'), may hold values from -6 to 6
- norm_gain: bfloat16 [4, 4096], P('section', 'dp'), may hold values from 0.5 to 1.5
- key_weight: bfloat16 [4, 4096, 512], P('section', 'dp'), may hold values from -0.09375 to 0.09375
- value_weight: bfloat16 [4, 4096, 512], P('section', 'dp'), may hold values from -0.09375 to 0.09375
- plan: int32 [4, 2], P('section'), may hold values from 0 to 1, each once within a row
Outputs:
- grad_inputs: bfloat16 [4, 2, 512, 4096], P('section', None, 'dp')
- key_weight_grad: float32 [4, 4096, 512], P('section', 'dp')
- value_weight_grad: float32 [4, 4096, 512], P('section', 'dp')
- gain_grad: float32 [4, 4096], P('section', 'dp')
The draws below stay inside these ranges and needn't reach their ends.
Inputs may be any that keep to these rules, and one draw needn't show every extreme that they name: Each row of plan lists every micro-batch once.
All inputs are finite; a program needn't handle non-finite values.
Results may differ from the reference program's by a relative error of at most 0.03.
Values may be sent and summed in bfloat16 or wider, within the bound.
No kernel may reach another device: no remote copies, remote signals or barrier semaphores. Data moves between devices by JAX's collectives and lax.ppermute only.
A program may use at most 128 MiB of HBM per device.

```python
import math
import jax
import jax.numpy as jnp
from jax import lax

D = 4096
HEADS = 32
KV_HEADS = 4
HEAD_DIM = 128
KV = 512
GROUP = 8
MB = 2
TOK_DEV = 64
TOKENS = 512
N_SECTION = 4
N_DP = 8


def strengthened(drawn, stream_key, source, target, blocks, factor):
    def block_of(position):
        return (jnp.arange(drawn.shape[position]) // (drawn.shape[position] // blocks)).reshape((-1,) + (1,) * (drawn.ndim - 1 - position))

    near = jax.random.permutation(stream_key, blocks)[block_of(target)]
    second = (block_of(target) + blocks // 2) % blocks
    return jnp.where((block_of(source) == near) | (block_of(source) == second), factor * drawn, drawn)


def level_of(key, shape, cuts, low, largest):
    level = 1.0
    for position, blocks in cuts:
        heights = jax.random.uniform(jax.random.fold_in(jax.random.fold_in(key, 6), position), (blocks,), jnp.float32, low / len(cuts), largest / len(cuts))
        level = level * jnp.repeat(jnp.exp(heights), shape[position] // blocks).reshape((-1,) + (1,) * (len(shape) - 1 - position))
    return level


def normal_values(stream_key, dims, scale, limit, split=(), held_as=jnp.bfloat16):
    entries = scale * jax.random.normal(stream_key, dims, jnp.float32)
    if split:
        entries = entries * level_of(stream_key, dims, split, -0.22, 0.18)
    return jnp.clip(entries, -limit, limit).astype(held_as)


def noise_with(stream_key, extent, spread, most, split, heavy, kind=jnp.bfloat16):
    result = spread * jax.random.normal(stream_key, extent, jnp.float32)
    if split:
        result = result * level_of(stream_key, extent, split, -0.22, 0.18)
    return jnp.clip(strengthened(result, jax.random.fold_in(stream_key, 3), *heavy), -most, most).astype(kind)


def setup_inputs(seed: int = 0) -> dict:
    splits = jax.random.split(jax.random.key(seed), 7)
    return {
        "inputs": noise_with(splits[0], (N_SECTION, MB, TOKENS, D), 1.0, 6.0, ((0, 4), (2, 8)), (2, 3, 8, 2.0)),
        "cotangent": normal_values(splits[1], (MB, TOKENS, D), 1.0, 6.0, ((1, 8),)),
        "norm_gain": jnp.clip(1.0 + 0.1 * jax.random.normal(splits[2], (N_SECTION, D), jnp.float32), 0.5, 1.5).astype(jnp.bfloat16),
        "key_weight": normal_values(splits[3], (N_SECTION, D, KV), D ** -0.5, 0.09375, ((0, 4), (1, 8))),
        "value_weight": normal_values(splits[4], (N_SECTION, D, KV), D ** -0.5, 0.09375, ((0, 4), (1, 8))),
        "plan": jax.vmap(lambda own: jax.random.permutation(own, MB))(jax.random.split(splits[5], N_SECTION)).reshape((N_SECTION, MB)).astype(jnp.int32),
    }


eps = 1e-05
rope_base = 500000.0

def rope_tables(length, head_dim):
    half_dim = head_dim // 2
    frequency = rope_base ** (-(jnp.arange(half_dim, dtype=jnp.float32) * 2.0 / head_dim))
    angles = jnp.arange(length, dtype=jnp.float32)[:, None] * frequency[None, :]
    cosine = jnp.concatenate([jnp.cos(angles), jnp.cos(angles)], axis=-1)
    sine_tab = jnp.concatenate([jnp.sin(angles), jnp.sin(angles)], axis=-1)
    return (cosine[:, None, :], sine_tab[:, None, :])

def turned(values):
    half_dim = values.shape[-1] // 2
    return jnp.concatenate([-values[..., half_dim:], values[..., :half_dim]], axis=-1)

def rotate(values, cosine, sine_tab):
    return values * cosine + turned(values) * sine_tab

def unrotate(values, cosine, sine_tab):
    return values * cosine - turned(values) * sine_tab

def forward(x_rows, gain, w_key, w_value):
    batch_count = x_rows.shape[0]
    length = x_rows.shape[1]
    score_scale = 1.0 / math.sqrt(HEAD_DIM)
    widened = x_rows.astype(jnp.float32)
    inv_rms = lax.rsqrt(lax.optimization_barrier(jnp.mean(widened * widened, axis=-1, keepdims=True)) + eps)
    gain_full = gain.astype(jnp.float32)
    normed = (widened * inv_rms * gain_full).astype(jnp.bfloat16)
    flat_normed = normed.reshape(batch_count * length, D)
    key_pre = jnp.dot(flat_normed, w_key, preferred_element_type=jnp.float32).reshape(batch_count, length, KV_HEADS, HEAD_DIM)
    value_heads = jnp.dot(flat_normed, w_value, preferred_element_type=jnp.float32).astype(jnp.bfloat16).reshape(batch_count, length, KV_HEADS, HEAD_DIM)
    cosine, sine_tab = rope_tables(length, HEAD_DIM)
    key_rot = rotate(key_pre, cosine, sine_tab).astype(jnp.bfloat16)
    query_rot = rotate(normed.astype(jnp.float32).reshape(batch_count, length, HEADS, HEAD_DIM), cosine, sine_tab).astype(jnp.bfloat16)
    query_rot = query_rot.reshape(batch_count, length, KV_HEADS, GROUP, HEAD_DIM)
    scores = jnp.einsum('blkgd,bmkd->bkglm', query_rot.astype(jnp.float32), key_rot.astype(jnp.float32)) * score_scale
    causal = jnp.arange(length)[:, None] >= jnp.arange(length)[None, :]
    raised = jnp.where(causal, jnp.exp(scores), 0.0)
    attn_prob = raised / lax.optimization_barrier(jnp.sum(raised, axis=-1, keepdims=True))
    prob_low = attn_prob.astype(jnp.bfloat16)
    return (widened, inv_rms, normed, query_rot, key_rot, value_heads, attn_prob, prob_low)

def backward(upper_grad, widened, inv_rms, normed, query_rot, key_rot, value_heads, attn_prob, prob_low, gain, w_key, w_value):
    batch_count = upper_grad.shape[0]
    length = upper_grad.shape[1]
    score_scale = 1.0 / math.sqrt(HEAD_DIM)
    grad_heads = upper_grad.astype(jnp.float32).reshape(batch_count, length, KV_HEADS, GROUP, HEAD_DIM)
    grad_prob = jnp.einsum('blkgd,bmkd->bkglm', grad_heads, value_heads.astype(jnp.float32))
    grad_value = jnp.einsum('bkglm,blkgd->bmkd', prob_low.astype(jnp.float32), grad_heads).astype(jnp.bfloat16)
    row_dot = lax.optimization_barrier(jnp.sum(attn_prob * grad_prob, axis=-1, keepdims=True))
    grad_score = (attn_prob * (grad_prob - row_dot) * score_scale).astype(jnp.bfloat16)
    grad_query = jnp.einsum('bkglm,bmkd->blkgd', grad_score.astype(jnp.float32), key_rot.astype(jnp.float32))
    grad_key = jnp.einsum('bkglm,blkgd->bmkd', grad_score.astype(jnp.float32), query_rot.astype(jnp.float32))
    cosine, sine_tab = rope_tables(length, HEAD_DIM)
    query_back = unrotate(grad_query.reshape(batch_count, length, HEADS, HEAD_DIM), cosine, sine_tab).reshape(batch_count, length, D)
    key_back = unrotate(grad_key, cosine, sine_tab).astype(jnp.bfloat16).reshape(batch_count * length, KV)
    value_flat = grad_value.reshape(batch_count * length, KV)
    projected_back = jnp.dot(key_back, w_key.T, preferred_element_type=jnp.float32) + jnp.dot(value_flat, w_value.T, preferred_element_type=jnp.float32)
    grad_normed = query_back + projected_back.reshape(batch_count, length, D)
    gain_full = gain.astype(jnp.float32)
    gain_term = grad_normed * widened * inv_rms
    projected = lax.optimization_barrier(jnp.mean(gain_term * gain_full, axis=-1, keepdims=True))
    lower_grad = upper_grad.astype(jnp.float32) + inv_rms * gain_full * grad_normed - widened * inv_rms * inv_rms * projected
    return (lower_grad.astype(jnp.bfloat16), key_back, value_flat, gain_term)

def regroup(array):
    return array.reshape(MB, N_DP, TOK_DEV, -1).transpose(1, 0, 2, 3).reshape(N_DP, MB * TOK_DEV, -1)

def add_group(totals, pieces):
    normed, key_back, value_flat, gain_term = pieces
    sum_key = jnp.dot(normed.T, key_back, preferred_element_type=jnp.float32)
    sum_value = jnp.dot(normed.T, value_flat, preferred_element_type=jnp.float32)
    sum_gain = lax.optimization_barrier(jnp.sum(gain_term, axis=0))
    rounded_key = lax.optimization_barrier(sum_key.astype(jnp.bfloat16)).astype(jnp.float32)
    rounded_value = lax.optimization_barrier(sum_value.astype(jnp.bfloat16)).astype(jnp.float32)
    rounded_gain = lax.optimization_barrier(sum_gain.astype(jnp.bfloat16)).astype(jnp.float32)
    return ((totals[0] + rounded_key, totals[1] + rounded_value, totals[2] + rounded_gain), None)

def reference(inputs, cotangent, norm_gain, key_weight, value_weight, plan):
    upper_grad = cotangent.reshape(MB * N_DP, TOK_DEV, D)
    grad_list = [None] * N_SECTION
    key_list = [None] * N_SECTION
    value_list = [None] * N_SECTION
    gain_list = [None] * N_SECTION
    for section_index in range(N_SECTION - 1, -1, -1):
        x_rows = inputs[section_index].reshape(MB * N_DP, TOK_DEV, D)
        saved = forward(x_rows, norm_gain[section_index], key_weight[section_index], value_weight[section_index])
        lower_grad, key_back, value_flat, gain_term = backward(upper_grad, *saved, norm_gain[section_index], key_weight[section_index], value_weight[section_index])
        normed = saved[2]
        start = (jnp.zeros((D, KV), jnp.float32), jnp.zeros((D, KV), jnp.float32), jnp.zeros((D,), jnp.float32))
        totals, unused = lax.scan(add_group, start, (regroup(normed), regroup(key_back), regroup(value_flat), regroup(gain_term)))
        key_list[section_index] = totals[0]
        value_list[section_index] = totals[1]
        gain_list[section_index] = totals[2]
        blocks = lower_grad.reshape(MB, TOKENS, D)
        grad_list[section_index] = blocks[plan[section_index]]
        upper_grad = lower_grad
    return (jnp.stack(grad_list), jnp.stack(key_list), jnp.stack(value_list), jnp.stack(gain_list))
```

```python
import functools
import math

import jax
import jax.numpy as jnp
from jax import lax
from jax.experimental import pallas as pl
from jax.experimental.pallas import tpu as pltpu
from jax.sharding import PartitionSpec as P


HEAD_DIM = 128
CHUNKS = 2
GAIN_ROWS = 16
BLOCK = 512

eps = 1e-05
rope_base = 500000.0
F32 = jnp.float32
BF16 = jnp.bfloat16
NT = (((1,), (1,)), ((), ()))
TN = (((0,), (0,)), ((), ()))
VMEM = pl.BlockSpec(memory_space=pltpu.VMEM)
SMEM = pl.BlockSpec(memory_space=pltpu.SMEM)
ANY = pl.BlockSpec(memory_space=pl.ANY)


def params(mib=40):
    return pltpu.CompilerParams(vmem_limit_bytes=mib * 1024 * 1024)


def cost(flops, size):
    return pl.CostEstimate(flops=int(flops), bytes_accessed=int(size), transcendentals=0)


def rope_tables(length):
    half = HEAD_DIM // 2
    frequency = rope_base ** (-(jnp.arange(half, dtype=F32) * 2.0 / HEAD_DIM))
    angles = jnp.arange(length, dtype=F32)[:, None] * frequency[None, :]
    cosine = jnp.concatenate([jnp.cos(angles), jnp.cos(angles)], axis=-1)
    sine = jnp.concatenate([-jnp.sin(angles), jnp.sin(angles)], axis=-1)
    return cosine, sine


def rotate(v, cosine, sine):
    return v * cosine + pltpu.roll(v, HEAD_DIM // 2, 1) * sine


def unrotate(v, cosine, sine):
    return v * cosine - pltpu.roll(v, HEAD_DIM // 2, 1) * sine


def head(i):
    return slice(i * HEAD_DIM, (i + 1) * HEAD_DIM)


def norm_kernel(batches, x_ref, gain_ref, cos_ref, sin_ref, normed_ref, query_ref, inv_ref):
    rows, width = x_ref.shape
    tok = rows // batches
    x = x_ref[...].astype(F32)
    inv = lax.rsqrt(jnp.mean(x * x, axis=-1, keepdims=True) + eps)
    inv_ref[...] = jnp.broadcast_to(inv, inv_ref.shape)
    for b in range(batches):
        r = slice(b * tok, (b + 1) * tok)
        inv_b = inv[r]
        for h in range(width // HEAD_DIM):
            v = (x_ref[r, head(h)].astype(F32) * inv_b * gain_ref[:, head(h)]).astype(BF16)
            normed_ref[r, head(h)] = v
            query_ref[r, head(h)] = rotate(v.astype(F32), cos_ref[...], sin_ref[...]).astype(BF16)


def assemble(lines, place_ref, pieces, out_ref, sem):
    z, c = place_ref[0], place_ref[1]
    size = pieces[0].shape[0]
    for side in range(2):
        core = c if side == 0 else 1 - c
        base = side * (2 * lines - 1)
        for k in range(lines):
            for sign in (1, -1):
                if k == 0 and sign == -1:
                    continue
                piece = pieces[base + (k if sign == 1 else lines - 1 + k)]
                place = z + sign * k

                @pl.when((place >= 0) & (place < lines))
                def _():
                    at = pl.multiple_of((2 * place + core) * size, size)
                    pltpu.make_async_copy(piece, out_ref.at[pl.ds(at, size)], sem).start()

    pltpu.make_async_copy(out_ref, out_ref, sem).wait()


def key_kernel(batches, chunks, lines, *refs):
    place_ref, normed_ref, query_ref, cos_ref, sin_ref = refs[:5]
    count = 2 * (2 * lines - 1)
    pieces = refs[5 : 5 + count]
    weight_ref, key_ref, prob_ref, sem = refs[5 + count :]
    assemble(lines, place_ref, pieces, weight_ref, sem)
    rows, width = normed_ref.shape
    tok = rows // batches
    part = tok // chunks
    key_heads = key_ref.shape[1] // HEAD_DIM
    group = width // HEAD_DIM // key_heads
    scale = 1.0 / math.sqrt(HEAD_DIM)
    pre = jnp.dot(normed_ref[...], weight_ref[...], preferred_element_type=F32)
    row = lax.broadcasted_iota(jnp.int32, (group * part, tok), 0) % part
    col = lax.broadcasted_iota(jnp.int32, (group * part, tok), 1)
    for b in range(batches):
        r = slice(b * tok, (b + 1) * tok)
        for k in range(key_heads):
            key = rotate(pre[r, head(k)], cos_ref[...], sin_ref[...]).astype(BF16)
            key_ref[r, head(k)] = key
            for j in range(chunks):
                rj = slice(b * tok + j * part, b * tok + (j + 1) * part)
                query = jnp.concatenate(
                    [query_ref[rj, head(k * group + g)] for g in range(group)], axis=0
                )
                scores = lax.dot_general(query, key, NT, preferred_element_type=F32) * scale
                raised = jnp.where(row + j * part >= col, jnp.exp(scores), 0.0)
                prob_ref[b, j, k] = raised / jnp.sum(raised, axis=-1, keepdims=True)


def value_kernel(lines, *refs):
    place_ref, normed_ref = refs[:2]
    count = 2 * (2 * lines - 1)
    pieces = refs[2 : 2 + count]
    weight_ref, value_ref, sem = refs[2 + count :]
    assemble(lines, place_ref, pieces, weight_ref, sem)
    value_ref[...] = jnp.dot(
        normed_ref[...], weight_ref[...], preferred_element_type=F32
    ).astype(BF16)


def turn_kernel(
    todo_ref,
    recv_ref,
    cot_ref,
    x_ref,
    inv_ref,
    gain_ref,
    query_ref,
    key_ref,
    value_ref,
    prob_ref,
    cos_ref,
    sin_ref,
    kw_ref,
    vw_ref,
    acc_in_ref,
    gsum_in_ref,
    grads_in_ref,
    kv_in_ref,
    lower_ref,
    acc_ref,
    gsum_ref,
    grads_ref,
    kv_ref,
    gn_ref,
    kvs_ref,
    gs_ref,
    sems,
):
    del grads_in_ref, kv_in_ref
    active, batch, chunk, last, slot, first = (todo_ref[i] for i in range(6))
    part, width = recv_ref.shape
    tok = key_ref.shape[1]
    kv_width = key_ref.shape[2]
    key_heads = kv_width // HEAD_DIM
    group = width // HEAD_DIM // key_heads
    scale = 1.0 / math.sqrt(HEAD_DIM)
    start = pl.multiple_of(chunk * part, part)

    @pl.when(active == 0)
    def _():
        gsum_ref[...] = gsum_in_ref[...]
        acc_ref[...] = acc_in_ref[...]

    @pl.when(active != 0)
    def _():
        cosine, sine = cos_ref[...], sin_ref[...]
        is_last = last != 0
        inv = inv_ref[:, :1]

        @pl.when(is_last)
        def _():
            lower_ref[...] = cot_ref[0]

        @pl.when(jnp.logical_not(is_last))
        def _():
            lower_ref[...] = recv_ref[...]

        keep = jnp.where(first != 0, 0.0, 1.0)
        for k in range(key_heads):
            upper = jnp.concatenate(
                [lower_ref[:, head(k * group + g)] for g in range(group)], axis=0
            )
            query = jnp.concatenate(
                [query_ref[0, :, head(k * group + g)] for g in range(group)], axis=0
            )
            key = key_ref[0, :, head(k)]
            prob = prob_ref[0, 0, k]
            grad_prob = lax.dot_general(
                upper, value_ref[0, :, head(k)], NT, preferred_element_type=F32
            )
            row_dot = jnp.sum(prob * grad_prob, axis=-1, keepdims=True)
            grad_score = (prob * (grad_prob - row_dot) * scale).astype(BF16)
            grad_query = jnp.dot(grad_score, key, preferred_element_type=F32)
            grad_key = lax.dot_general(grad_score, query, TN, preferred_element_type=F32)
            grad_value = lax.dot_general(
                prob.astype(BF16), upper, TN, preferred_element_type=F32
            )
            kc = head(k)
            vc = slice(kv_width + k * HEAD_DIM, kv_width + (k + 1) * HEAD_DIM)
            old_key = jnp.where(keep > 0.0, acc_in_ref[:, kc], 0.0)
            old_value = jnp.where(keep > 0.0, acc_in_ref[:, vc], 0.0)
            acc_ref[:, kc] = old_key + grad_key
            acc_ref[:, vc] = old_value + grad_value
            kvs_ref[:, kc] = unrotate(
                acc_ref[pl.ds(start, part), kc], cosine, sine
            ).astype(BF16)
            kvs_ref[:, vc] = acc_ref[pl.ds(start, part), vc].astype(BF16)
            for g in range(group):
                gn_ref[:, head(k * group + g)] = unrotate(
                    grad_query[g * part : (g + 1) * part], cosine, sine
                )
        kv_copy = pltpu.make_async_copy(
            kvs_ref, kv_ref.at[batch, pl.ds(start, part)], sems.at[0]
        )
        kv_copy.start()
        projected = jnp.zeros((part, HEAD_DIM), F32)
        key_back, value_back = kvs_ref[:, :kv_width], kvs_ref[:, kv_width:]
        for i in range(width // BLOCK):
            s = slice(i * BLOCK, (i + 1) * BLOCK)
            grad_normed = gn_ref[:, s] + (
                lax.dot_general(key_back, kw_ref[s], NT, preferred_element_type=F32)
                + lax.dot_general(value_back, vw_ref[s], NT, preferred_element_type=F32)
            )
            gn_ref[:, s] = grad_normed
            term = grad_normed * x_ref[0, :, s].astype(F32) * inv
            for r in range(0, part, 8):
                if r == 0:
                    folded = term[:8]
                else:
                    folded = folded + term[r : r + 8]
            gsum_ref[:, s] = gsum_in_ref[:, s] + folded
            scaled = term * gain_ref[:, s]
            for q in range(BLOCK // HEAD_DIM):
                projected = projected + scaled[:, head(q)]
        projected = jnp.sum(projected, axis=-1, keepdims=True) * (1.0 / width)
        pull = inv * inv * projected
        for i in range(width // BLOCK):
            s = slice(i * BLOCK, (i + 1) * BLOCK)
            lower = (
                lower_ref[:, s].astype(F32)
                + inv * gain_ref[:, s] * gn_ref[:, s]
                - x_ref[0, :, s].astype(F32) * pull
            )
            lower_ref[:, s] = lower.astype(BF16)
        total = jnp.sum(gsum_ref[...], axis=0, keepdims=True).astype(BF16)
        wide = 2 * kv_width
        for i in range(width // wide):
            gs_ref[i : i + 1, :] = total[:, i * wide : (i + 1) * wide]
        gain_copy = pltpu.make_async_copy(
            gs_ref, kv_ref.at[batch, pl.ds(tok, GAIN_ROWS)], sems.at[1]
        )
        gain_copy.start()
        out_copy = pltpu.make_async_copy(
            lower_ref, grads_ref.at[slot, pl.ds(start, part)], sems.at[2]
        )
        out_copy.start()
        kv_copy.wait()
        gain_copy.wait()
        out_copy.wait()


def weight_kernel(tok, last, *refs):
    place_ref, x_own, x_other = refs[:3]
    batch = refs[-1]
    own_kv, other_kv = refs[3:5]
    rows = own_kv.shape[0]
    x = jnp.concatenate(
        [x_own[k] for k in range(rows)] + [x_other[k] for k in range(rows)], axis=0
    )
    kv = jnp.concatenate(
        [own_kv[k, :tok] for k in range(rows)] + [other_kv[k, :tok] for k in range(rows)], axis=0
    )
    del batch
    product = lax.dot_general(x, kv, TN, preferred_element_type=F32)
    if not last:
        refs[5][...] = product
        return
    partial_ref, key_out, value_out, gain_out = refs[5:9]
    product = product + partial_ref[...]
    half = product.shape[1] // 2
    key_out[...] = product[:, :half]
    value_out[...] = product[:, half:]
    z, c = place_ref[0], place_ref[1]
    size = gain_out.shape[1]
    per_row = own_kv.shape[2] // size
    index = 2 * z + c
    total = jnp.zeros((1, size), F32)
    for i in range(own_kv.shape[1] - tok):
        for j in range(per_row):
            mine = jnp.zeros((1, size), F32)
            if i * per_row + j >= partial_ref.shape[0] * 0 + 2 * rows:
                continue
            cols = slice(j * size, (j + 1) * size)
            for k in range(rows):
                mine = mine + own_kv[k, tok + i : tok + i + 1, cols].astype(F32)
                mine = mine + other_kv[k, tok + i : tok + i + 1, cols].astype(F32)
            total = jnp.where(index == i * per_row + j, mine, total)
    gain_out[...] = total


def after(value, *others):
    return lax.optimization_barrier((value,) + others)[0]


def body(inputs, cotangent, norm_gain, key_weight, value_weight, plan):
    sections = lax.axis_size("section")
    lines = lax.axis_size("dp") // 2
    section_index = lax.axis_index("section")
    dp_index = lax.axis_index("dp")
    z, c = dp_index // 2, dp_index % 2
    place = jnp.stack([z, c]).astype(jnp.int32)
    _, batches, tok, width = inputs.shape
    own, kv_width = key_weight.shape[1:]
    key_heads = kv_width // HEAD_DIM
    group = width // HEAD_DIM // key_heads
    chunks = CHUNKS
    part = tok // chunks
    units = batches * chunks
    rows = batches * tok

    def along(value, pairs):
        return lax.ppermute(
            value, "dp", [(2 * a + core, 2 * b + core) for a, b in pairs for core in range(2)]
        )

    def swap(value, held=None):
        held = range(lines) if held is None else held
        return lax.ppermute(
            value, "dp", [(2 * a + core, 2 * a + 1 - core) for a in held for core in range(2)]
        )

    def shifted(value, k):
        return along(value, [(a, (a + k) % lines) for a in range(lines)])

    up = {"k": [key_weight[0]], "v": [value_weight[0]]}
    down = {"k": [key_weight[0]], "v": [value_weight[0]]}
    for k in range(1, lines):
        for name in ("k", "v"):
            up[name].append(along(up[name][-1], [(a + 1, a) for a in range(lines - k)]))
            down[name].append(along(down[name][-1], [(a, a + 1) for a in range(k - 1, lines - 1)]))
    pieces = {}
    for name in ("k", "v"):
        mine = up[name] + down[name][1:]
        other = [swap(up[name][k], range(lines - k)) for k in range(lines)]
        other += [swap(down[name][k], range(k, lines)) for k in range(1, lines)]
        pieces[name] = mine + other

    gain_own = jnp.stack([norm_gain] + [shifted(norm_gain, -k) for k in range(1, lines)])
    gain_other = swap(gain_own)
    first = jnp.where(c == 0, gain_own, gain_other)
    second = jnp.where(c == 0, gain_other, gain_own)
    gains = jnp.concatenate([first, second], axis=1)
    gains = jnp.roll(gains, z, axis=0).reshape(1, width).astype(F32)

    cosine, sine = rope_tables(tok)
    x_rows = inputs[0]
    normed, query, inv = pl.pallas_call(
        functools.partial(norm_kernel, batches),
        out_shape=(
            jax.ShapeDtypeStruct((rows, width), BF16),
            jax.ShapeDtypeStruct((rows, width), BF16),
            jax.ShapeDtypeStruct((rows, HEAD_DIM), F32),
        ),
        in_specs=[VMEM] * 4,
        out_specs=(VMEM,) * 3,
        compiler_params=params(),
        cost_estimate=cost(2e9, 4 * rows * width),
        name="norm",
    )(x_rows.reshape(rows, width), gains, cosine, sine)

    count = len(pieces["k"])
    key_full, key, prob = pl.pallas_call(
        functools.partial(key_kernel, batches, chunks, lines),
        out_shape=(
            jax.ShapeDtypeStruct((width, kv_width), BF16),
            jax.ShapeDtypeStruct((rows, kv_width), BF16),
            jax.ShapeDtypeStruct((batches, chunks, key_heads, group * part, tok), F32),
        ),
        in_specs=[SMEM] + [VMEM] * 4 + [ANY] * count,
        out_specs=(VMEM,) * 3,
        scratch_shapes=[pltpu.SemaphoreType.DMA],
        compiler_params=params(),
        cost_estimate=cost(2 * rows * width * kv_width, 2 * width * kv_width),
        name="keys",
    )(place, normed, query, cosine, sine, *pieces["k"])

    value_full, value = pl.pallas_call(
        functools.partial(value_kernel, lines),
        out_shape=(
            jax.ShapeDtypeStruct((width, kv_width), BF16),
            jax.ShapeDtypeStruct((rows, kv_width), BF16),
        ),
        in_specs=[SMEM] + [VMEM] + [ANY] * count,
        out_specs=(VMEM,) * 2,
        scratch_shapes=[pltpu.SemaphoreType.DMA],
        compiler_params=params(),
        cost_estimate=cost(2 * rows * width * kv_width, 2 * width * kv_width),
        name="values",
    )(place, normed, *pieces["v"])

    def blocked(array):
        return array.reshape(batches, tok, array.shape[-1])

    key, value, query = blocked(key), blocked(value), blocked(query)
    kv_rows = tok + GAIN_ROWS
    wide = 2 * kv_width
    acc = jnp.zeros((tok, wide), F32)
    gsum = jnp.zeros((8, width), F32)
    grads = jnp.zeros((batches, tok, width), BF16)
    kv = jnp.zeros((batches, kv_rows, wide), BF16)
    slots = jnp.argmax(
        plan[0][None, :] == jnp.arange(batches, dtype=jnp.int32)[:, None], axis=1
    ).astype(jnp.int32)
    is_last = (section_index == sections - 1).astype(jnp.int32)

    def by_unit(*shape):
        return pl.BlockSpec(shape, lambda i, t: (t[1], t[2]) + (0,) * (len(shape) - 2))

    def by_batch(*shape):
        return pl.BlockSpec(shape, lambda i, t: (t[1],) + (0,) * (len(shape) - 1))

    turn_call = pl.pallas_call(
        turn_kernel,
        grid_spec=pltpu.PrefetchScalarGridSpec(
            num_scalar_prefetch=1,
            grid=(1,),
            in_specs=[
                VMEM,
                by_unit(1, part, width),
                by_unit(1, part, width),
                pl.BlockSpec((part, HEAD_DIM), lambda i, t: (t[1] * chunks + t[2], 0)),
                VMEM,
                by_unit(1, part, width),
                by_batch(1, tok, kv_width),
                by_batch(1, tok, kv_width),
                by_unit(1, 1, key_heads, group * part, tok),
                pl.BlockSpec((part, HEAD_DIM), lambda i, t: (t[2], 0)),
                pl.BlockSpec((part, HEAD_DIM), lambda i, t: (t[2], 0)),
                VMEM,
                VMEM,
                VMEM,
                VMEM,
                ANY,
                ANY,
            ],
            out_specs=(VMEM, VMEM, VMEM, ANY, ANY),
            scratch_shapes=[
                pltpu.VMEM((part, width), F32),
                pltpu.VMEM((part, wide), BF16),
                pltpu.VMEM((GAIN_ROWS, wide), BF16),
                pltpu.SemaphoreType.DMA((3,)),
            ],
        ),
        out_shape=(
            jax.ShapeDtypeStruct((part, width), BF16),
            jax.ShapeDtypeStruct(acc.shape, F32),
            jax.ShapeDtypeStruct(gsum.shape, F32),
            jax.ShapeDtypeStruct(grads.shape, BF16),
            jax.ShapeDtypeStruct(kv.shape, BF16),
        ),
        input_output_aliases={14: 1, 15: 2, 16: 3, 17: 4},
        compiler_params=params(),
        cost_estimate=cost(2 * part * width * wide * 8, 2 * width * wide),
        name="turn",
    )

    x_by_chip = normed.reshape(batches, tok, lines, 2 * own)
    gathered = {}

    def x_part(k):
        at = (z + k) % lines
        return lax.dynamic_index_in_dim(x_by_chip, at, 2, keepdims=False)

    x_parts = [None] * lines
    turns = units + 2 * (sections - 1)
    sent = [jnp.zeros((part, width), BF16)] * 2
    for turn in range(turns):
        unit = turn - 2 * (sections - 1 - section_index)
        active = (unit >= 0) & (unit < units)
        unit = jnp.clip(unit, 0, units - 1)
        batch = unit // chunks
        chunk = chunks - 1 - unit % chunks
        slot = jnp.sum(jnp.where(jnp.arange(batches) == batch, slots, 0))
        todo = jnp.stack(
            [active.astype(jnp.int32), batch, chunk, is_last, slot, (unit % chunks == 0)]
        ).astype(jnp.int32)
        lower, acc, gsum, grads, kv = turn_call(
            todo,
            sent[-2],
            cotangent,
            inputs[0],
            inv,
            gains,
            query,
            key,
            value,
            prob,
            cosine,
            sine,
            key_full,
            value_full,
            acc,
            gsum,
            grads,
            kv,
        )
        pairs = [
            (s, s - 1)
            for s in range(1, sections)
            if 0 <= turn - 2 * (sections - 1 - s) < units
        ]
        sent.append(lax.ppermute(lower, "section", pairs) if pairs else sent[0])
        if turn < lines:
            piece = after(x_part(turn), lower)
            x_parts[turn] = shifted(piece, turn) if turn else piece
        for b in range(batches):
            if turn == 2 * (sections - 1) + (b + 1) * chunks - 1:
                message = kv[b] if b == batches - 1 else kv[b, :tok]
                mine = jnp.stack([message] + [shifted(message, k) for k in range(1, lines)])
                gathered[b] = (mine, swap(mine))

    for k in range(turns, lines):
        x_parts[k] = shifted(x_part(k), k)
    x_all = jnp.stack(x_parts)
    x_own = lax.dynamic_slice_in_dim(x_all, c * own, own, 3)
    x_other = swap(lax.dynamic_slice_in_dim(x_all, (1 - c) * own, own, 3))

    flops = 2 * 2 * lines * tok * own * wide
    partial = None
    for b in range(batches):
        last = b == batches - 1
        operands = [place, x_own[:, b], x_other[:, b], *gathered[b]]
        if not last:
            out = jax.ShapeDtypeStruct((own, wide), F32)
            result = pl.pallas_call(
                lambda *refs: weight_kernel(tok, False, *refs, None),
                out_shape=out,
                in_specs=[SMEM] + [VMEM] * 4,
                out_specs=VMEM,
                compiler_params=params(),
                cost_estimate=cost(flops, 4 * own * wide),
                name="weights",
            )(*operands)
            partial = result if partial is None else partial + result
    if partial is None:
        partial = jnp.zeros((own, wide), F32)
    key_grad, value_grad, gain_grad = pl.pallas_call(
        lambda *refs: weight_kernel(tok, True, *refs, None),
        out_shape=(
            jax.ShapeDtypeStruct((own, kv_width), F32),
            jax.ShapeDtypeStruct((own, kv_width), F32),
            jax.ShapeDtypeStruct((1, own), F32),
        ),
        in_specs=[SMEM] + [VMEM] * 5,
        out_specs=(VMEM,) * 3,
        compiler_params=params(),
        cost_estimate=cost(flops, 4 * own * wide),
        name="weights_last",
    )(*operands, partial)
    return (grads[None], key_grad[None], value_grad[None], gain_grad)


def solution(mesh):
    in_specs = (
        P("section", None, "dp", None),
        P(None, "dp", None),
        P("section", "dp"),
        P("section", "dp", None),
        P("section", "dp", None),
        P("section", None),
    )
    out_specs = (
        P("section", None, "dp", None),
        P("section", "dp", None),
        P("section", "dp", None),
        P("section", "dp"),
    )
    return jax.shard_map(body, mesh=mesh, in_specs=in_specs, out_specs=out_specs, check_vma=False)
```

```python
import functools
import math

import jax
import jax.numpy as jnp
from jax import lax
from jax.experimental import pallas as pl
from jax.experimental.pallas import tpu as pltpu
from jax.sharding import PartitionSpec as P


HEAD_DIM = 128
CHUNKS = 2
GAIN_ROWS = 8
BLOCK = 512
TURN_MIB = 24

eps = 1e-05
rope_base = 500000.0
F32 = jnp.float32
BF16 = jnp.bfloat16
NT = (((1,), (1,)), ((), ()))
TN = (((0,), (0,)), ((), ()))
VMEM = pl.BlockSpec(memory_space=pltpu.VMEM)
SMEM = pl.BlockSpec(memory_space=pltpu.SMEM)
ANY = pl.BlockSpec(memory_space=pl.ANY)
HBM = pl.BlockSpec(memory_space=pltpu.HBM)
HALF_OUT = VMEM


def params(mib=40):
    return pltpu.CompilerParams(vmem_limit_bytes=mib * 1024 * 1024)


def cost(flops, size):
    return pl.CostEstimate(flops=int(flops), bytes_accessed=int(size), transcendentals=0)


def rope_tables(length):
    half = HEAD_DIM // 2
    frequency = rope_base ** (-(jnp.arange(half, dtype=F32) * 2.0 / HEAD_DIM))
    angles = jnp.arange(length, dtype=F32)[:, None] * frequency[None, :]
    cosine = jnp.concatenate([jnp.cos(angles), jnp.cos(angles)], axis=-1)
    sine = jnp.concatenate([-jnp.sin(angles), jnp.sin(angles)], axis=-1)
    return cosine, sine


def rotate(v, cosine, sine):
    return v * cosine + pltpu.roll(v, HEAD_DIM // 2, 1) * sine


def unrotate(v, cosine, sine):
    return v * cosine - pltpu.roll(v, HEAD_DIM // 2, 1) * sine


def head(i):
    return slice(i * HEAD_DIM, (i + 1) * HEAD_DIM)


def norm_kernel(batches, lines, place_ref, x_ref, own_ref, other_ref, cos_ref, sin_ref, *outs):
    normed_ref, query_ref, inv_ref, gain_ref, gsum_ref = outs[:5]
    part_refs = outs[5 : 5 + lines]
    rows, width = x_ref.shape
    tok = rows // batches
    z, c = place_ref[0], place_ref[1]
    own = own_ref.shape[2]
    for k in range(lines):
        chip = lax.rem(z + k, lines)
        for core, ref in ((c, own_ref), (1 - c, other_ref)):
            at = pl.multiple_of((2 * chip + core) * own, own)
            gain_ref[:, pl.ds(at, own)] = ref[k].astype(F32)
    x = x_ref[...].astype(F32)
    inv = lax.rsqrt(jnp.mean(x * x, axis=-1, keepdims=True) + eps)
    inv_ref[...] = jnp.broadcast_to(inv, inv_ref.shape)
    gsum_ref[...] = jnp.zeros_like(gsum_ref)

    def one(h, carry):
        at = pl.ds(pl.multiple_of(h * HEAD_DIM, HEAD_DIM), HEAD_DIM)
        for b in range(batches):
            r = slice(b * tok, (b + 1) * tok)
            v = (x_ref[r, at].astype(F32) * inv_ref[r, :1] * gain_ref[:, at]).astype(BF16)
            normed_ref[r, at] = v
            query_ref[r, at] = rotate(v.astype(F32), cos_ref[...], sin_ref[...]).astype(BF16)
        return carry

    lax.fori_loop(0, width // HEAD_DIM, one, 0)
    for k in range(lines):
        at = pl.multiple_of(lax.rem(z + k, lines) * 2 * own, 2 * own)
        part_refs[k][...] = normed_ref[:, pl.ds(at, 2 * own)]


def pack_kernel(place_ref, *refs):
    own_ref, other_ref = refs[-2:]
    own = own_ref.shape[2]
    c = place_ref[1]
    for k, ref in enumerate(refs[:-2]):
        own_ref[k] = ref[:, pl.ds(pl.multiple_of(c * own, own), own)]
        other_ref[k] = ref[:, pl.ds(pl.multiple_of((1 - c) * own, own), own)]


def half_kernel(lines, place_ref, *refs):
    pieces, (out_ref, sem) = refs[:-2], refs[-2:]
    z = place_ref[0]

    def copies():
        for k in range(lines - 1):
            for sign in (1, -1):
                if k == 0 and sign == -1:
                    continue
                piece = pieces[k if sign == 1 else lines - 2 + k]
                at = z + sign * k
                yield (at >= 0) & (at < lines), pltpu.make_async_copy(
                    piece, out_ref.at[jnp.clip(at, 0, lines - 1)], sem
                )

    for wanted, copy in copies():
        pl.when(wanted)(copy.start)
    for wanted, copy in copies():
        pl.when(wanted)(copy.wait)


def merge(lines, place_ref, own_ref, other_ref, late, out_ref, sems):
    z, c = place_ref[0], place_ref[1]
    far = lines - 1
    for core, half, ups in ((c, own_ref, late[:2]), (1 - c, other_ref, late[2:])):
        for chip in range(lines):
            late_here = jnp.bool_(False)
            if chip == far:
                late_here = z == 0
            if chip == 0:
                late_here = z == far

            @pl.when(jnp.logical_not(late_here))
            def _():
                pltpu.make_async_copy(half.at[chip], out_ref.at[chip, core], sems).start()

        for chip, here, piece in ((far, 0, ups[0]), (0, far, ups[1])):

            @pl.when(z == here)
            def _():
                pltpu.make_async_copy(piece, out_ref.at[chip, core], sems).start()

    pltpu.make_async_copy(out_ref, out_ref, sems).wait()


def project(normed_ref, weight_ref):
    lines, _, own, columns = weight_ref.shape
    total = jnp.zeros((normed_ref.shape[0], columns), F32)
    for i in range(lines):
        for c in range(2):
            at = (2 * i + c) * own
            total = total + jnp.dot(
                normed_ref[:, at : at + own], weight_ref[i, c], preferred_element_type=F32
            )
    return total


def key_kernel(batches, chunks, lines, *refs):
    place_ref, normed_ref, query_ref, cos_ref, sin_ref, own_ref, other_ref = refs[:7]
    weight_ref, key_ref, prob_ref, sems = refs[11:]
    merge(lines, place_ref, own_ref, other_ref, refs[7:11], weight_ref, sems)
    rows, width = normed_ref.shape
    tok = rows // batches
    part = tok // chunks
    key_heads = key_ref.shape[1] // HEAD_DIM
    group = width // HEAD_DIM // key_heads
    scale = 1.0 / math.sqrt(HEAD_DIM)
    pre = project(normed_ref, weight_ref)
    for b in range(batches):
        r = slice(b * tok, (b + 1) * tok)
        for k in range(key_heads):
            key_ref[r, head(k)] = rotate(pre[r, head(k)], cos_ref[...], sin_ref[...]).astype(BF16)
    row = lax.broadcasted_iota(jnp.int32, (group * part, tok), 0) % part
    col = lax.broadcasted_iota(jnp.int32, (group * part, tok), 1)

    def one(bk, carry):
        b, k = bk // key_heads, bk % key_heads
        rows_b = pl.ds(pl.multiple_of(b * tok, tok), tok)
        key = key_ref[rows_b, pl.ds(pl.multiple_of(k * HEAD_DIM, HEAD_DIM), HEAD_DIM)]
        for j in range(chunks):
            rj = pl.ds(pl.multiple_of(b * tok + j * part, part), part)
            query = jnp.concatenate(
                [
                    query_ref[rj, pl.ds(pl.multiple_of((k * group + g) * HEAD_DIM, HEAD_DIM), HEAD_DIM)]
                    for g in range(group)
                ],
                axis=0,
            )
            scores = lax.dot_general(query, key, NT, preferred_element_type=F32) * scale
            raised = jnp.where(row + j * part >= col, jnp.exp(scores), 0.0)
            prob_ref[b, j, k] = raised / jnp.sum(raised, axis=-1, keepdims=True)
        return carry

    lax.fori_loop(0, batches * key_heads, one, 0)


def value_kernel(lines, place_ref, normed_ref, own_ref, other_ref, *refs):
    weight_ref, value_ref, sems = refs[4:]
    merge(lines, place_ref, own_ref, other_ref, refs[:4], weight_ref, sems)
    value_ref[...] = project(normed_ref, weight_ref).astype(BF16)


def turn_kernel(
    turn,
    sections,
    chunks,
    info_ref,
    inv_ref,
    gain_ref,
    key_ref,
    value_ref,
    cos_ref,
    sin_ref,
    acc_in_ref,
    gsum_in_ref,
    cot_ref,
    x_all_ref,
    query_all_ref,
    prob_ref,
    kw_ref,
    vw_ref,
    recv_hbm,
    grads_in_ref,
    *refs,
):
    del grads_in_ref
    batches, tok, _ = x_all_ref.shape
    lower_ref, acc_ref, gsum_ref, grads_ref = refs[batches : batches + 4]
    kv_refs = refs[batches + 4 : 2 * batches + 4]
    up_ref, gn_ref, kvs_ref, gs_ref, in_sem, out_sems = refs[2 * batches + 4 :]
    part, width = up_ref.shape
    kv_width = key_ref.shape[1]
    key_heads = kv_width // HEAD_DIM
    group = width // HEAD_DIM // key_heads
    scale = 1.0 / math.sqrt(HEAD_DIM)
    section = info_ref[0]
    unit = turn - 2 * (sections - 1 - section)
    active = (unit >= 0) & (unit < batches * chunks)
    is_last = section == sections - 1
    blocks = width // BLOCK

    @pl.when(jnp.logical_not(active))
    def _():
        gsum_ref[...] = gsum_in_ref[...]
        acc_ref[...] = acc_in_ref[...]

    @pl.when(active)
    def _():
        batch = unit // chunks
        fresh = unit % chunks
        chunk = chunks - 1 - fresh
        start = pl.multiple_of(chunk * part, part)
        row = pl.multiple_of(batch * tok + chunk * part, part)
        rows_b = pl.ds(pl.multiple_of(batch * tok, tok), tok)
        slot = info_ref[1 + batch]
        here = pl.ds(start, part)

        @pl.when(is_last)
        def _():
            up_ref[...] = cot_ref[batch, here]

        @pl.when(jnp.logical_not(is_last))
        def _():
            copy = pltpu.make_async_copy(recv_hbm, up_ref, in_sem)
            copy.start()
            copy.wait()

        cosine, sine = cos_ref[here], sin_ref[here]
        inv = inv_ref[pl.ds(row, part), :1]
        for k in range(key_heads):
            upper = jnp.concatenate(
                [up_ref[:, head(k * group + g)] for g in range(group)], axis=0
            )
            query = jnp.concatenate(
                [query_all_ref[batch, here, head(k * group + g)] for g in range(group)], axis=0
            )
            key = key_ref[rows_b, head(k)]
            prob = prob_ref[batch, chunk, k]
            grad_prob = lax.dot_general(
                upper, value_ref[rows_b, head(k)], NT, preferred_element_type=F32
            )
            row_dot = jnp.sum(prob * grad_prob, axis=-1, keepdims=True)
            grad_score = (prob * (grad_prob - row_dot) * scale).astype(BF16)
            grad_query = jnp.dot(grad_score, key, preferred_element_type=F32)
            grad_key = lax.dot_general(grad_score, query, TN, preferred_element_type=F32)
            grad_value = lax.dot_general(
                prob.astype(BF16), upper, TN, preferred_element_type=F32
            )
            kc = head(k)
            vc = slice(kv_width + k * HEAD_DIM, kv_width + (k + 1) * HEAD_DIM)
            acc_ref[:, kc] = jnp.where(fresh == 0, 0.0, acc_in_ref[:, kc]) + grad_key
            acc_ref[:, vc] = jnp.where(fresh == 0, 0.0, acc_in_ref[:, vc]) + grad_value
            kvs_ref[:, kc] = unrotate(acc_ref[here, kc], cosine, sine).astype(BF16)
            kvs_ref[:, vc] = acc_ref[here, vc].astype(BF16)
            for g in range(group):
                gn_ref[:, head(k * group + g)] = unrotate(
                    grad_query[g * part : (g + 1) * part], cosine, sine
                )
        for b in range(batches):

            @pl.when(batch == b)
            def _():
                pltpu.make_async_copy(kvs_ref, kv_refs[b].at[here], out_sems.at[0]).start()

        projected = jnp.zeros((part, HEAD_DIM), F32)
        key_back, value_back = kvs_ref[:, :kv_width], kvs_ref[:, kv_width:]
        for i in range(blocks):
            s = slice(i * BLOCK, (i + 1) * BLOCK)
            grad_normed = gn_ref[:, s] + (
                lax.dot_general(key_back, kw_ref[s], NT, preferred_element_type=F32)
                + lax.dot_general(value_back, vw_ref[s], NT, preferred_element_type=F32)
            )
            gn_ref[:, s] = grad_normed
            term = grad_normed * x_all_ref[batch, here, s].astype(F32) * inv
            folded = term[:8]
            for r in range(8, part, 8):
                folded = folded + term[r : r + 8]
            gsum_ref[:, s] = gsum_in_ref[:, s] + folded
            scaled = term * gain_ref[:, s]
            for q in range(BLOCK // HEAD_DIM):
                projected = projected + scaled[:, head(q)]
        projected = jnp.sum(projected, axis=-1, keepdims=True) * (1.0 / width)
        pull = inv * inv * projected
        for i in range(blocks):
            s = slice(i * BLOCK, (i + 1) * BLOCK)
            lower = (
                up_ref[:, s].astype(F32)
                + inv * gain_ref[:, s] * gn_ref[:, s]
                - x_all_ref[batch, here, s].astype(F32) * pull
            )
            lower_ref[:, s] = lower.astype(BF16)
        out_copy = pltpu.make_async_copy(lower_ref, grads_ref.at[slot, here], out_sems.at[2])
        out_copy.start()
        total = jnp.sum(gsum_ref[...], axis=0, keepdims=True).astype(BF16)
        wide = 2 * kv_width
        for i in range(width // wide):
            gs_ref[i : i + 1, :] = total[:, i * wide : (i + 1) * wide]
        end = pl.ds(tok, GAIN_ROWS)
        for b in range(batches):

            @pl.when(batch == b)
            def _():
                pltpu.make_async_copy(gs_ref, kv_refs[b].at[end], out_sems.at[1]).start()

        pltpu.make_async_copy(kvs_ref, kv_refs[0].at[here], out_sems.at[0]).wait()
        pltpu.make_async_copy(gs_ref, kv_refs[0].at[end], out_sems.at[1]).wait()
        out_copy.wait()


def weight_sum(xs, kvs):
    x = jnp.concatenate(xs, axis=0)
    kv = jnp.concatenate(kvs, axis=0)
    return lax.dot_general(x, kv, TN, preferred_element_type=F32)


def weight_kernel(tok, lines, batches, *refs):
    x_own, x_other, kvs, out_ref = refs[0], refs[1], refs[2:-1], refs[-1]
    xs, gs, at = [], [], 0
    for b in range(batches):
        for x_ref in (x_own, x_other) if b < batches - 1 else (x_own,):
            for k in range(lines):
                xs.append(x_ref[k, b * tok : (b + 1) * tok])
                gs.append(kvs[at][:tok])
                at += 1
    out_ref[...] = weight_sum(xs, gs)


def weight_last_kernel(tok, lines, batches, place_ref, x_ref, partial_ref, *refs):
    own_kv, other_kv = refs[:lines], refs[lines : 2 * lines]
    key_out, value_out, gain_out = refs[2 * lines :]
    last = slice((batches - 1) * tok, batches * tok)
    product = partial_ref[...] + weight_sum(
        [x_ref[k, last] for k in range(lines)], [ref[:tok] for ref in other_kv]
    )
    half = product.shape[1] // 2
    key_out[...] = product[:, :half]
    value_out[...] = product[:, half:]
    size = gain_out.shape[1]
    per_row = product.shape[1] // size
    index = 2 * place_ref[0] + place_ref[1]
    total = jnp.zeros((1, size), F32)
    for i in range(2 * lines):
        at = slice(tok + i // per_row, tok + i // per_row + 1)
        cols = slice(i % per_row * size, (i % per_row + 1) * size)
        mine = jnp.zeros((1, size), F32)
        for ref in own_kv + other_kv:
            mine = mine + ref[at, cols].astype(F32)
        total = jnp.where(index == i, mine, total)
    gain_out[...] = total


def after(value, *others):
    return lax.optimization_barrier((value,) + others)[0]


def body(inputs, cotangent, norm_gain, key_weight, value_weight, plan):
    sections = lax.axis_size("section")
    lines = lax.axis_size("dp") // 2
    section_index = lax.axis_index("section")
    dp_index = lax.axis_index("dp")
    z, c = dp_index // 2, dp_index % 2
    place = jnp.stack([z, c]).astype(jnp.int32)
    _, batches, tok, width = inputs.shape
    own, kv_width = key_weight.shape[1:]
    key_heads = kv_width // HEAD_DIM
    group = width // HEAD_DIM // key_heads
    chunks = CHUNKS
    part = tok // chunks
    units = batches * chunks
    rows = batches * tok

    def along(value, pairs):
        return lax.ppermute(
            value, "dp", [(2 * a + core, 2 * b + core) for a, b in pairs for core in range(2)]
        )

    def swap(value, held=None):
        held = range(lines) if held is None else held
        return lax.ppermute(
            value, "dp", [(2 * a + core, 2 * a + 1 - core) for a in held for core in range(2)]
        )

    def shifted(value, k):
        return along(value, [(a, (a + k) % lines) for a in range(lines)])

    gain_own = jnp.stack([norm_gain] + [shifted(norm_gain, -k) for k in range(1, lines)])
    gain_other = swap(gain_own)

    cosine, sine = rope_tables(tok)
    x_rows = inputs[0]
    kv_rows = tok + GAIN_ROWS
    wide = 2 * kv_width
    outs = pl.pallas_call(
        functools.partial(norm_kernel, batches, lines),
        out_shape=(
            jax.ShapeDtypeStruct((rows, width), BF16),
            jax.ShapeDtypeStruct((rows, width), BF16),
            jax.ShapeDtypeStruct((rows, HEAD_DIM), F32),
            jax.ShapeDtypeStruct((1, width), F32),
            jax.ShapeDtypeStruct((8, width), F32),
            *[jax.ShapeDtypeStruct((rows, 2 * own), BF16)] * lines,
            jax.ShapeDtypeStruct((tok, wide), F32),
            jax.ShapeDtypeStruct((batches, tok, width), BF16),
            *[jax.ShapeDtypeStruct((kv_rows, wide), BF16)] * batches,
        ),
        in_specs=[SMEM] + [VMEM] * 5,
        out_specs=(VMEM,) * (5 + lines) + (ANY, HBM) + (HBM,) * batches,
        compiler_params=params(16),
        cost_estimate=cost(2e9, 4 * rows * width),
        name="norm",
    )(place, x_rows.reshape(rows, width), gain_own, gain_other, cosine, sine)
    normed, query, inv, gains, gsum = outs[:5]
    x_send = outs[5 : 5 + lines]
    acc, grads = outs[5 + lines : 7 + lines]
    kvs = outs[7 + lines :]

    names = ("k", "v")
    up = {"k": [key_weight[0]], "v": [value_weight[0]]}
    down = {"k": [key_weight[0]], "v": [value_weight[0]]}
    for k in range(1, lines):
        for name in names:
            above, below = up[name][-1], down[name][-1]
            if k == 2 and name == "v":
                above, below = after(above, gain_other), after(below, gain_other)
            if k == lines - 1 and k > 1 and name == "k":
                above, below = after(above, inv), after(below, inv)
            up[name].append(along(above, [(a + 1, a) for a in range(lines - k)]))
            down[name].append(along(below, [(a, a + 1) for a in range(k - 1, lines - 1)]))

    def halves(name):
        mine = pl.pallas_call(
            functools.partial(half_kernel, lines),
            out_shape=jax.ShapeDtypeStruct((lines, own, kv_width), BF16),
            in_specs=[SMEM] + [ANY] * (2 * lines - 3),
            out_specs=HALF_OUT,
            scratch_shapes=[pltpu.SemaphoreType.DMA],
            compiler_params=params(8),
            cost_estimate=cost(1e9, 2 * lines * own * kv_width),
            name="half",
        )(place, *up[name][:-1], *down[name][1:-1])
        return mine, swap(mine)

    half = {name: halves(name) for name in names}
    late = {}
    key_full, key, prob = None, None, None
    late["k"] = [up["k"][-1], down["k"][-1]]
    late["k"] += [swap(late["k"][0], [0]), swap(late["k"][1], [lines - 1])]
    late["k"][0] = after(late["k"][0], half["v"][0])
    key_full, key, prob = pl.pallas_call(
        functools.partial(key_kernel, batches, chunks, lines),
        out_shape=(
            jax.ShapeDtypeStruct((lines, 2, own, kv_width), BF16),
            jax.ShapeDtypeStruct((rows, kv_width), BF16),
            jax.ShapeDtypeStruct((batches, chunks, key_heads, group * part, tok), F32),
        ),
        in_specs=[SMEM] + [VMEM] * 4 + [ANY] * 6,
        out_specs=(VMEM,) * 3,
        scratch_shapes=[pltpu.SemaphoreType.DMA],
        compiler_params=params(24),
        cost_estimate=cost(2 * rows * width * kv_width, 2 * width * kv_width),
        name="keys",
    )(place, normed, query, cosine, sine, *half["k"], *late["k"])

    late["v"] = [after(up["v"][-1], key), after(down["v"][-1], key)]
    late["v"] += [swap(late["v"][0], [0]), swap(late["v"][1], [lines - 1])]
    value_full, value = pl.pallas_call(
        functools.partial(value_kernel, lines),
        out_shape=(
            jax.ShapeDtypeStruct((lines, 2, own, kv_width), BF16),
            jax.ShapeDtypeStruct((rows, kv_width), BF16),
        ),
        in_specs=[SMEM] + [VMEM] + [ANY] * 6,
        out_specs=(VMEM,) * 2,
        scratch_shapes=[pltpu.SemaphoreType.DMA],
        compiler_params=params(16),
        cost_estimate=cost(2 * rows * width * kv_width, 2 * width * kv_width),
        name="values",
    )(place, normed, *half["v"], *late["v"])
    key_full = key_full.reshape(width, kv_width)
    value_full = value_full.reshape(width, kv_width)

    query = query.reshape(batches, tok, width)
    batch_of = jnp.arange(batches, dtype=jnp.int32)
    slots = jnp.sum(
        jnp.where(plan[0][None, :] == batch_of[:, None], batch_of[None, :], 0), axis=1
    ).astype(jnp.int32)
    info = jnp.concatenate([section_index.astype(jnp.int32)[None], slots])

    recv0 = jnp.zeros((part, width), BF16)

    def turn_call(turn, *operands):
        return pl.pallas_call(
            functools.partial(turn_kernel, turn, sections, chunks),
            out_shape=(
                jax.ShapeDtypeStruct((part, width), BF16),
                jax.ShapeDtypeStruct(acc.shape, F32),
                jax.ShapeDtypeStruct(gsum.shape, F32),
                jax.ShapeDtypeStruct(grads.shape, BF16),
                *[jax.ShapeDtypeStruct((kv_rows, wide), BF16)] * batches,
            ),
            in_specs=[SMEM] + [VMEM] * 14 + [ANY] + [HBM] * (1 + batches),
            out_specs=(VMEM, VMEM, VMEM, HBM) + (HBM,) * batches,
            scratch_shapes=[
                pltpu.VMEM((part, width), BF16),
                pltpu.VMEM((part, width), F32),
                pltpu.VMEM((part, wide), BF16),
                pltpu.VMEM((GAIN_ROWS, wide), BF16),
                pltpu.SemaphoreType.DMA,
                pltpu.SemaphoreType.DMA((3,)),
            ],
            input_output_aliases={7: 1, 8: 2, 16: 3} | {17 + b: 4 + b for b in range(batches)},
            compiler_params=params(TURN_MIB),
            cost_estimate=cost(2 * part * width * wide * 8, 2 * width * wide),
            name="turn",
        )(*operands)

    gathered = {}
    x_recv = {0: x_send[0]}
    x_own = x_other = None
    units_from = 2 * (sections - 1)
    turns = units + units_from
    sent = [recv0, recv0]

    def pack():
        own_part, other_part = pl.pallas_call(
            pack_kernel,
            out_shape=(jax.ShapeDtypeStruct((lines, rows, own), BF16),) * 2,
            in_specs=[SMEM] + [VMEM] * lines,
            out_specs=(VMEM,) * 2,
            compiler_params=params(8),
            cost_estimate=cost(1e8, 4 * lines * rows * own),
            name="pack",
        )(place, *[x_recv[k] for k in range(lines)])
        return own_part, swap(other_part)

    for turn in range(turns):
        recv = sent[-2]
        if turn == units_from:
            x_own, x_other = pack()
            recv = after(recv, x_own)
        if turn == turns - 1 and batches > 1:
            recv = after(recv, *gathered[batches - 2][:lines])
        lower, acc, gsum, grads, *kvs = turn_call(
            turn,
            info,
            inv,
            gains,
            key,
            value,
            cosine,
            sine,
            acc,
            gsum,
            cotangent,
            inputs[0],
            query,
            prob,
            key_full,
            value_full,
            recv,
            grads,
            *kvs,
        )
        pairs = [
            (s, s - 1)
            for s in range(1, sections)
            if 0 <= turn - 2 * (sections - 1 - s) < units
        ]
        sent.append(lax.ppermute(lower, "section", pairs) if pairs else recv0)
        many = range(1, lines) if turn == units_from - 2 else [turn - 1]
        for k in many:
            if 1 <= k < lines and k not in x_recv and turn < units_from - 1:
                x_recv[k] = shifted(after(x_send[k], lower), k)
        for b in range(batches):
            if turn == units_from + (b + 1) * chunks - 1:
                mine = [kvs[b]] + [shifted(kvs[b], k) for k in range(1, lines)]
                gathered[b] = mine + [swap(m) for m in mine]

    flops = 2 * 2 * lines * tok * own * wide
    final = batches - 1
    operands = [kv for b in range(final) for kv in gathered[b]] + gathered[final][:lines]
    partial = pl.pallas_call(
        functools.partial(weight_kernel, tok, lines, batches),
        out_shape=jax.ShapeDtypeStruct((own, wide), F32),
        in_specs=[VMEM] * (2 + len(operands)),
        out_specs=VMEM,
        compiler_params=params(24),
        cost_estimate=cost(flops, 4 * own * wide),
        name="weights",
    )(x_own, x_other, *operands)
    key_grad, value_grad, gain_grad = pl.pallas_call(
        functools.partial(weight_last_kernel, tok, lines, batches),
        out_shape=(
            jax.ShapeDtypeStruct((own, kv_width), F32),
            jax.ShapeDtypeStruct((own, kv_width), F32),
            jax.ShapeDtypeStruct((1, own), F32),
        ),
        in_specs=[SMEM] + [VMEM] * (2 + 2 * lines),
        out_specs=(VMEM,) * 3,
        compiler_params=params(24),
        cost_estimate=cost(flops, 4 * own * wide),
        name="weights_last",
    )(place, x_other, partial, *gathered[final])
    return (grads[None], key_grad[None], value_grad[None], gain_grad)


def solution(mesh):
    in_specs = (
        P("section", None, "dp", None),
        P(None, "dp", None),
        P("section", "dp"),
        P("section", "dp", None),
        P("section", "dp", None),
        P("section", None),
    )
    out_specs = (
        P("section", None, "dp", None),
        P("section", "dp", None),
        P("section", "dp", None),
        P("section", "dp"),
    )
    return jax.shard_map(body, mesh=mesh, in_specs=in_specs, out_specs=out_specs, check_vma=False)
```

```python
import functools
import math

import jax
import jax.numpy as jnp
from jax import lax
from jax.experimental import pallas as pl
from jax.experimental.pallas import tpu as pltpu
from jax.sharding import PartitionSpec as P


HEAD_DIM = 128
CHUNKS = 2
GAIN_ROWS = 8
BLOCK = 512
TURN_MIB = 24

eps = 1e-05
rope_base = 500000.0
F32 = jnp.float32
BF16 = jnp.bfloat16
NT = (((1,), (1,)), ((), ()))
TN = (((0,), (0,)), ((), ()))
VMEM = pl.BlockSpec(memory_space=pltpu.VMEM)
SMEM = pl.BlockSpec(memory_space=pltpu.SMEM)
ANY = pl.BlockSpec(memory_space=pl.ANY)
HBM = pl.BlockSpec(memory_space=pltpu.HBM)
HALF_OUT = VMEM


def params(mib=40):
    return pltpu.CompilerParams(vmem_limit_bytes=mib * 1024 * 1024)


def cost(flops, size):
    return pl.CostEstimate(flops=int(flops), bytes_accessed=int(size), transcendentals=0)


def rope_tables(length):
    half = HEAD_DIM // 2
    frequency = rope_base ** (-(jnp.arange(half, dtype=F32) * 2.0 / HEAD_DIM))
    angles = jnp.arange(length, dtype=F32)[:, None] * frequency[None, :]
    cosine = jnp.concatenate([jnp.cos(angles), jnp.cos(angles)], axis=-1)
    sine = jnp.concatenate([-jnp.sin(angles), jnp.sin(angles)], axis=-1)
    return cosine, sine


def rotate(v, cosine, sine):
    return v * cosine + pltpu.roll(v, HEAD_DIM // 2, 1) * sine


def unrotate(v, cosine, sine):
    return v * cosine - pltpu.roll(v, HEAD_DIM // 2, 1) * sine


def head(i):
    return slice(i * HEAD_DIM, (i + 1) * HEAD_DIM)


def norm_kernel(batches, lines, place_ref, x_ref, own_ref, other_ref, cos_ref, sin_ref, *outs):
    normed_ref, query_ref, inv_ref, gain_ref, gsum_ref = outs[:5]
    part_refs = outs[5 : 5 + lines]
    rows, width = x_ref.shape
    tok = rows // batches
    z, c = place_ref[0], place_ref[1]
    own = own_ref.shape[2]
    for k in range(lines):
        chip = lax.rem(z + k, lines)
        for core, ref in ((c, own_ref), (1 - c, other_ref)):
            at = pl.multiple_of((2 * chip + core) * own, own)
            gain_ref[:, pl.ds(at, own)] = ref[k].astype(F32)
    x = x_ref[...].astype(F32)
    inv = lax.rsqrt(jnp.mean(x * x, axis=-1, keepdims=True) + eps)
    inv_ref[...] = jnp.broadcast_to(inv, inv_ref.shape)
    gsum_ref[...] = jnp.zeros_like(gsum_ref)

    def one(h, carry):
        at = pl.ds(pl.multiple_of(h * HEAD_DIM, HEAD_DIM), HEAD_DIM)
        for b in range(batches):
            r = slice(b * tok, (b + 1) * tok)
            v = (x_ref[r, at].astype(F32) * inv_ref[r, :1] * gain_ref[:, at]).astype(BF16)
            normed_ref[r, at] = v
            query_ref[r, at] = rotate(v.astype(F32), cos_ref[...], sin_ref[...]).astype(BF16)
        return carry

    lax.fori_loop(0, width // HEAD_DIM, one, 0, unroll=8)
    for k in range(lines):
        at = pl.multiple_of(lax.rem(z + k, lines) * 2 * own, 2 * own)
        part_refs[k][...] = normed_ref[:, pl.ds(at, 2 * own)]


def pack_kernel(place_ref, mine_ref, *refs):
    own_ref, other_ref = refs[-2:]
    own = own_ref.shape[2]
    c = place_ref[1]
    count = len(refs[:-2]) // 2
    limit = place_ref[place_ref.shape[0] - 1]
    for way in range(2):

        @pl.when((place_ref[2] < limit) == (way == 0))
        def _():
            pack(c, own, (mine_ref,) + refs[way * count : (way + 1) * count], own_ref, other_ref)


def pack(c, own, refs, own_ref, other_ref):
    for k, ref in enumerate(refs):
        own_ref[k] = ref[:, pl.ds(pl.multiple_of(c * own, own), own)]
        other_ref[k] = ref[:, pl.ds(pl.multiple_of((1 - c) * own, own), own)]


def half_kernel(lines, place_ref, *refs):
    pieces, (out_ref, held_ref, sem) = refs[:-3], refs[-3:]
    z = place_ref[0]
    half = lines // 2
    lower = z < half
    m = jnp.where(lower, z, lines - 1 - z)
    sign = jnp.where(lower, 1, -1)

    def copies():
        todo = [(m >= 0, z)]
        todo += [((m <= min(half - 2, lines - 1 - k)), z + sign * k) for k in range(1, lines - 1)]
        todo += [(m == half - 1, z + sign * k) for k in range(1, half + 1)]
        todo += [(m >= k, z - sign * k) for k in range(1, half)]
        for piece, (wanted, at) in zip(pieces, todo):
            yield wanted, pltpu.make_async_copy(
                piece, held_ref.at[jnp.clip(at, 0, lines - 1)], sem
            )

    for wanted, copy in copies():
        pl.when(wanted)(copy.start)
    for wanted, copy in copies():
        pl.when(wanted)(copy.wait)

    def one(i, carry):
        out_ref[i] = held_ref[i].T
        return carry

    lax.fori_loop(0, lines, one, 0)


def merge_kernel(lines, place_ref, normed_ref, own_ref, other_ref, out_ref, partial_ref, sems):
    z, c = place_ref[0], place_ref[1]
    own = own_ref.shape[2]
    copies = []
    for chip in range(lines):
        for core, half in ((c, own_ref), (1 - c, other_ref)):
            at = pl.multiple_of((2 * chip + core) * own, own)
            copies.append(
                pltpu.make_async_copy(half.at[chip], out_ref.at[:, pl.ds(at, own)], sems)
            )
    for copy in copies:
        copy.start()
    for copy in copies:
        copy.wait()
    total = jnp.zeros(partial_ref.shape, F32)
    for chip in range(lines):
        at = slice(2 * chip * own, 2 * (chip + 1) * own)
        product = lax.dot_general(
            normed_ref[:, at], out_ref[:, at], NT, preferred_element_type=F32
        )
        if chip in (0, lines - 1):
            missing = z == lines - 1 - chip
            product = jnp.where(missing, 0.0, product)
        total = total + product
    partial_ref[...] = total


def finish(lines, place_ref, normed_ref, partial_ref, late, out_ref, held_ref, turned_ref, sems):
    z, c = place_ref[0], place_ref[1]
    far = lines - 1
    own = held_ref.shape[1]
    for chip, here in ((far, 0), (0, far)):

        @pl.when(z == here)
        def _():
            loads = [
                pltpu.make_async_copy(piece, held_ref.at[i], sems.at[i])
                for i, piece in enumerate(late)
            ]
            stores = []
            for load in loads:
                load.start()
            for i, core in enumerate((c, 1 - c)):
                loads[i].wait()
                turned_ref[i] = held_ref[i].T
                at = pl.ds(pl.multiple_of((2 * chip + core) * own, own), own)
                stores.append(
                    pltpu.make_async_copy(turned_ref.at[i], out_ref.at[:, at], sems.at[2 + i])
                )
                stores[-1].start()
                partial_ref[...] += jnp.dot(
                    normed_ref[:, at], held_ref[i], preferred_element_type=F32
                )
            for store in stores:
                store.wait()


def key_kernel(batches, chunks, lines, *refs):
    place_ref, normed_ref, query_ref, cos_ref, sin_ref, partial_ref, _ = refs[:7]
    weight_ref, key_ref, prob_ref, pre_ref, held_ref, turned_ref, sems = refs[9:]
    pre_ref[...] = partial_ref[...]
    finish(lines, place_ref, normed_ref, pre_ref, refs[7:9], weight_ref, held_ref, turned_ref, sems)
    rows, width = normed_ref.shape
    tok = rows // batches
    part = tok // chunks
    key_heads = key_ref.shape[1] // HEAD_DIM
    group = width // HEAD_DIM // key_heads
    scale = 1.0 / math.sqrt(HEAD_DIM)
    for b in range(batches):
        r = slice(b * tok, (b + 1) * tok)
        for k in range(key_heads):
            key_ref[r, head(k)] = rotate(
                pre_ref[r, head(k)], cos_ref[...], sin_ref[...]
            ).astype(BF16)
    row = lax.broadcasted_iota(jnp.int32, (group * part, tok), 0) % part
    col = lax.broadcasted_iota(jnp.int32, (group * part, tok), 1)

    def one(bk, carry):
        b, k = bk // key_heads, bk % key_heads
        rows_b = pl.ds(pl.multiple_of(b * tok, tok), tok)
        key = key_ref[rows_b, pl.ds(pl.multiple_of(k * HEAD_DIM, HEAD_DIM), HEAD_DIM)]
        for j in range(chunks):
            rj = pl.ds(pl.multiple_of(b * tok + j * part, part), part)
            query = jnp.concatenate(
                [
                    query_ref[rj, pl.ds(pl.multiple_of((k * group + g) * HEAD_DIM, HEAD_DIM), HEAD_DIM)]
                    for g in range(group)
                ],
                axis=0,
            )
            scores = lax.dot_general(query, key, NT, preferred_element_type=F32) * scale
            raised = jnp.where(row + j * part >= col, jnp.exp(scores), 0.0)
            prob_ref[b, j, k] = raised / jnp.sum(raised, axis=-1, keepdims=True)
        return carry

    lax.fori_loop(0, batches * key_heads, one, 0)


def value_kernel(lines, place_ref, normed_ref, partial_ref, _, *refs):
    weight_ref, value_ref, pre_ref, held_ref, turned_ref, sems = refs[2:]
    pre_ref[...] = partial_ref[...]
    finish(lines, place_ref, normed_ref, pre_ref, refs[:2], weight_ref, held_ref, turned_ref, sems)
    value_ref[...] = pre_ref[...].astype(BF16)


def turn_kernel(
    turn,
    sections,
    chunks,
    left,
    info_ref,
    inv_ref,
    gain_ref,
    key_ref,
    value_ref,
    cos_ref,
    sin_ref,
    acc_in_ref,
    gsum_in_ref,
    cot_ref,
    x_all_ref,
    query_all_ref,
    prob_ref,
    kw_ref,
    vw_ref,
    recv_hbm,
    grads_in_ref,
    *refs,
):
    del grads_in_ref
    batches, tok, _ = x_all_ref.shape
    count = len(left)
    lower_ref, acc_ref, gsum_ref, grads_ref = refs[count : count + 4]
    kv_refs = dict(zip(left, refs[count + 4 : 2 * count + 4]))
    up_ref, gn_ref, kvs_ref, gs_ref, in_sem, out_sems = refs[2 * count + 4 :]
    part, width = up_ref.shape
    kv_width = key_ref.shape[1]
    key_heads = kv_width // HEAD_DIM
    group = width // HEAD_DIM // key_heads
    scale = 1.0 / math.sqrt(HEAD_DIM)
    section = info_ref[2]
    unit = turn - 2 * (sections - 1 - section)
    active = (unit >= 0) & (unit < batches * chunks)
    is_last = section == sections - 1
    blocks = width // BLOCK

    @pl.when(jnp.logical_not(active))
    def _():
        gsum_ref[...] = gsum_in_ref[...]
        acc_ref[...] = acc_in_ref[...]

    @pl.when(active)
    def _():
        batch = unit // chunks
        fresh = unit % chunks
        chunk = chunks - 1 - fresh
        start = pl.multiple_of(chunk * part, part)
        row = pl.multiple_of(batch * tok + chunk * part, part)
        rows_b = pl.ds(pl.multiple_of(batch * tok, tok), tok)
        slot = info_ref[3 + batch]
        here = pl.ds(start, part)

        @pl.when(is_last)
        def _():
            up_ref[...] = cot_ref[batch, here]

        @pl.when(jnp.logical_not(is_last))
        def _():
            copy = pltpu.make_async_copy(recv_hbm, up_ref, in_sem)
            copy.start()
            copy.wait()

        cosine, sine = cos_ref[here], sin_ref[here]
        inv = inv_ref[pl.ds(row, part), :1]

        def one(k, carry):
            def at(i):
                return pl.ds(pl.multiple_of(i * HEAD_DIM, HEAD_DIM), HEAD_DIM)

            upper = jnp.concatenate([up_ref[:, at(k * group + g)] for g in range(group)], axis=0)
            query = jnp.concatenate(
                [query_all_ref[batch, here, at(k * group + g)] for g in range(group)], axis=0
            )
            key = key_ref[rows_b, at(k)]
            prob = prob_ref[batch, chunk, k]
            grad_prob = lax.dot_general(
                upper, value_ref[rows_b, at(k)], NT, preferred_element_type=F32
            )
            row_dot = jnp.sum(prob * grad_prob, axis=-1, keepdims=True)
            grad_score = (prob * (grad_prob - row_dot) * scale).astype(BF16)
            grad_query = jnp.dot(grad_score, key, preferred_element_type=F32)
            grad_key = lax.dot_general(grad_score, query, TN, preferred_element_type=F32)
            grad_value = lax.dot_general(
                prob.astype(BF16), upper, TN, preferred_element_type=F32
            )
            kc, vc = at(k), at(key_heads + k)
            acc_ref[:, kc] = jnp.where(fresh == 0, 0.0, acc_in_ref[:, kc]) + grad_key
            acc_ref[:, vc] = jnp.where(fresh == 0, 0.0, acc_in_ref[:, vc]) + grad_value
            kvs_ref[:, kc] = unrotate(acc_ref[here, kc], cosine, sine).astype(BF16)
            kvs_ref[:, vc] = acc_ref[here, vc].astype(BF16)
            for g in range(group):
                gn_ref[:, at(k * group + g)] = unrotate(
                    grad_query[g * part : (g + 1) * part], cosine, sine
                )
            return carry

        lax.fori_loop(0, key_heads, one, 0, unroll=2)
        for b in left:

            @pl.when(batch == b)
            def _():
                pltpu.make_async_copy(kvs_ref, kv_refs[b].at[here], out_sems.at[0]).start()

        projected = jnp.zeros((part, HEAD_DIM), F32)
        key_back, value_back = kvs_ref[:, :kv_width], kvs_ref[:, kv_width:]
        for i in range(blocks):
            s = slice(i * BLOCK, (i + 1) * BLOCK)
            grad_normed = gn_ref[:, s] + (
                jnp.dot(key_back, kw_ref[:, s], preferred_element_type=F32)
                + jnp.dot(value_back, vw_ref[:, s], preferred_element_type=F32)
            )
            gn_ref[:, s] = grad_normed
            term = grad_normed * x_all_ref[batch, here, s].astype(F32) * inv
            folded = term[:8]
            for r in range(8, part, 8):
                folded = folded + term[r : r + 8]
            gsum_ref[:, s] = gsum_in_ref[:, s] + folded
            scaled = term * gain_ref[:, s]
            for q in range(BLOCK // HEAD_DIM):
                projected = projected + scaled[:, head(q)]
        projected = jnp.sum(projected, axis=-1, keepdims=True) * (1.0 / width)
        pull = inv * inv * projected
        for i in range(blocks):
            s = slice(i * BLOCK, (i + 1) * BLOCK)
            lower = (
                up_ref[:, s].astype(F32)
                + inv * gain_ref[:, s] * gn_ref[:, s]
                - x_all_ref[batch, here, s].astype(F32) * pull
            )
            lower_ref[:, s] = lower.astype(BF16)
        out_copy = pltpu.make_async_copy(lower_ref, grads_ref.at[slot, here], out_sems.at[2])
        out_copy.start()
        pltpu.make_async_copy(kvs_ref, kv_refs[left[0]].at[here], out_sems.at[0]).wait()

        @pl.when(unit == batches * chunks - 1)
        def _():
            total = jnp.sum(gsum_ref[...], axis=0, keepdims=True).astype(BF16)
            wide = 2 * kv_width
            for i in range(width // wide):
                gs_ref[i : i + 1, :] = total[:, i * wide : (i + 1) * wide]
            end = pl.ds(tok, GAIN_ROWS)
            gain_copy = pltpu.make_async_copy(
                gs_ref, kv_refs[batches - 1].at[end], out_sems.at[1]
            )
            gain_copy.start()
            gain_copy.wait()

        out_copy.wait()


def weight_sum(xs, kvs):
    x = jnp.concatenate(xs, axis=0)
    kv = jnp.concatenate(kvs, axis=0)
    return lax.dot_general(x, kv, TN, preferred_element_type=F32)


def weight_kernel(tok, lines, batches, *refs):
    x_own, x_other, kvs, out_ref = refs[0], refs[1], refs[2:-1], refs[-1]
    xs, gs, at = [], [], 0
    for b in range(batches):
        for x_ref in (x_own, x_other) if b < batches - 1 else (x_own,):
            for k in range(lines):
                xs.append(x_ref[k, b * tok : (b + 1) * tok])
                gs.append(kvs[at][:tok])
                at += 1
    out_ref[...] = weight_sum(xs, gs)


def weight_last_kernel(tok, lines, batches, place_ref, x_ref, partial_ref, *refs):
    own_kv, other_kv = refs[:lines], refs[lines : 2 * lines]
    key_out, value_out, gain_out = refs[2 * lines :]
    last = slice((batches - 1) * tok, batches * tok)
    product = partial_ref[...] + weight_sum(
        [x_ref[k, last] for k in range(lines)], [ref[:tok] for ref in other_kv]
    )
    half = product.shape[1] // 2
    key_out[...] = product[:, :half]
    value_out[...] = product[:, half:]
    size = gain_out.shape[1]
    per_row = product.shape[1] // size
    index = 2 * place_ref[0] + place_ref[1]
    total = jnp.zeros((1, size), F32)
    for i in range(2 * lines):
        at = slice(tok + i // per_row, tok + i // per_row + 1)
        cols = slice(i % per_row * size, (i % per_row + 1) * size)
        mine = jnp.zeros((1, size), F32)
        for ref in own_kv + other_kv:
            mine = mine + ref[at, cols].astype(F32)
        total = jnp.where(index == i, mine, total)
    gain_out[...] = total


def after(value, *others):
    return lax.optimization_barrier((value,) + others)[0]


def body(inputs, cotangent, norm_gain, key_weight, value_weight, plan):
    sections = lax.axis_size("section")
    lines = lax.axis_size("dp") // 2
    section_index = lax.axis_index("section")
    dp_index = lax.axis_index("dp")
    z, c = dp_index // 2, dp_index % 2
    _, batches, tok, width = inputs.shape
    batch_of = jnp.arange(batches, dtype=jnp.int32)
    slots = jnp.sum(
        jnp.where(plan[0][None, :] == batch_of[:, None], batch_of[None, :], 0), axis=1
    ).astype(jnp.int32)
    half_way = jnp.full((1,), sections - 1, jnp.int32)
    place = jnp.concatenate(
        [jnp.stack([z, c, section_index]).astype(jnp.int32), slots, half_way]
    )
    own, kv_width = key_weight.shape[1:]
    key_heads = kv_width // HEAD_DIM
    group = width // HEAD_DIM // key_heads
    chunks = CHUNKS
    part = tok // chunks
    units = batches * chunks
    rows = batches * tok

    def along(value, pairs):
        return lax.ppermute(
            value, "dp", [(2 * a + core, 2 * b + core) for a, b in pairs for core in range(2)]
        )

    def swap(value, held=None):
        held = range(lines) if held is None else held
        return lax.ppermute(
            value, "dp", [(2 * a + core, 2 * a + 1 - core) for a in held for core in range(2)]
        )

    def shifted(value, k):
        return along(value, [(a, (a + k) % lines) for a in range(lines)])

    gain_parts = [norm_gain]
    for k in range(1, lines):
        gain_parts.append(shifted(norm_gain, -k))
    gain_own = jnp.stack(gain_parts)
    gain_other = swap(gain_own)

    cosine, sine = rope_tables(tok)
    x_rows = inputs[0]
    kv_rows = [tok] * (batches - 1) + [tok + GAIN_ROWS]
    wide = 2 * kv_width
    outs = pl.pallas_call(
        functools.partial(norm_kernel, batches, lines),
        out_shape=(
            jax.ShapeDtypeStruct((rows, width), BF16),
            jax.ShapeDtypeStruct((rows, width), BF16),
            jax.ShapeDtypeStruct((rows, HEAD_DIM), F32),
            jax.ShapeDtypeStruct((1, width), F32),
            jax.ShapeDtypeStruct((8, width), F32),
            *[jax.ShapeDtypeStruct((rows, 2 * own), BF16)] * lines,
            jax.ShapeDtypeStruct((tok, wide), F32),
            jax.ShapeDtypeStruct((batches, tok, width), BF16),
            *[jax.ShapeDtypeStruct((kv_rows[b], wide), BF16) for b in range(batches)],
            jax.ShapeDtypeStruct((part, width), BF16),
        ),
        in_specs=[SMEM] + [VMEM] * 5,
        out_specs=(VMEM,) * (5 + lines) + (ANY, HBM) + (HBM,) * (batches + 1),
        compiler_params=params(16),
        cost_estimate=cost(2e9, 4 * rows * width),
        name="norm",
    )(place, x_rows.reshape(rows, width), gain_own, gain_other, cosine, sine)
    normed, query, inv, gains, gsum = outs[:5]
    x_send = outs[5 : 5 + lines]
    acc, grads = outs[5 + lines : 7 + lines]
    kvs = dict(enumerate(outs[7 + lines : 7 + lines + batches]))
    recv0 = outs[-1]

    names = ("k", "v")
    side = lines // 2

    def both(pairs):
        return pairs + [(lines - 1 - a, lines - 1 - b) for a, b in pairs]

    middle = (z == side - 1) | (z == side)
    shard = {"k": key_weight[0], "v": value_weight[0]}
    outward = {name: [] for name in names}
    across = {name: [] for name in names}
    inward = {name: [] for name in names}
    for k in range(1, lines):
        for name in names:
            if k == 1:
                from_middle = from_end = shard[name]
            else:
                from_middle = across[name][k - 2] if k - 2 < side else outward[name][k - 2]
                if side > 2:
                    crossed = across[name][min(k - 2, side - 1)]
                    from_middle = jnp.where(middle, crossed, outward[name][k - 2])
                from_end = inward[name][k - 2] if k - 2 < side - 1 else None
            ends = min(side - 2, lines - 1 - k)
            outward[name].append(along(from_middle, both([(m + 1, m) for m in range(ends + 1)])))
            if k <= side:
                across[name].append(along(from_end, both([(side, side - 1)])))
            if k < side:
                inward[name].append(along(from_end, both([(m - 1, m) for m in range(k, side)])))
    ends = [0, lines - 1]

    def halves(name):
        mine = pl.pallas_call(
            functools.partial(half_kernel, lines),
            out_shape=jax.ShapeDtypeStruct((lines, kv_width, own), BF16),
            in_specs=[SMEM] + [ANY] * (2 * lines - 2),
            out_specs=HALF_OUT,
            scratch_shapes=[
                pltpu.VMEM((lines, own, kv_width), BF16),
                pltpu.SemaphoreType.DMA,
            ],
            compiler_params=params(8),
            cost_estimate=cost(1e9, 2 * lines * own * kv_width),
        )(place, shard[name], *outward[name][:-1], *across[name], *inward[name])
        return mine, swap(mine)

    def merged(name):
        return pl.pallas_call(
            functools.partial(merge_kernel, lines),
            out_shape=(
                jax.ShapeDtypeStruct((kv_width, width), BF16),
                jax.ShapeDtypeStruct((rows, kv_width), F32),
            ),
            in_specs=[SMEM, VMEM, ANY, ANY],
            out_specs=(VMEM, VMEM),
            scratch_shapes=[pltpu.SemaphoreType.DMA],
            compiler_params=params(12),
            cost_estimate=cost(2 * rows * width * kv_width, 2 * width * kv_width),
        )(place, normed, *halves(name))

    whole = {name: merged(name) for name in names}
    late_scratch = [
        pltpu.VMEM((rows, kv_width), F32),
        pltpu.VMEM((2, own, kv_width), BF16),
        pltpu.VMEM((2, kv_width, own), BF16),
        pltpu.SemaphoreType.DMA((4,)),
    ]
    late = {}
    key_full, key, prob = None, None, None
    late["k"] = [outward["k"][-1]]
    late["k"].append(swap(late["k"][0], ends))
    key_full, key, prob = pl.pallas_call(
        functools.partial(key_kernel, batches, chunks, lines),
        out_shape=(
            jax.ShapeDtypeStruct((kv_width, width), BF16),
            jax.ShapeDtypeStruct((rows, kv_width), BF16),
            jax.ShapeDtypeStruct((batches, chunks, key_heads, group * part, tok), F32),
        ),
        in_specs=[SMEM] + [VMEM] * 5 + [ANY] * 3,
        out_specs=(ANY, VMEM, VMEM),
        scratch_shapes=late_scratch,
        input_output_aliases={6: 0},
        compiler_params=params(16),
        cost_estimate=cost(2 * rows * width * kv_width, 2 * width * kv_width),
        name="keys",
    )(place, normed, query, cosine, sine, whole["k"][1], whole["k"][0], *late["k"])

    late["v"] = [after(outward["v"][-1], key)]
    late["v"].append(swap(late["v"][0], ends))
    value_full, value = pl.pallas_call(
        functools.partial(value_kernel, lines),
        out_shape=(
            jax.ShapeDtypeStruct((kv_width, width), BF16),
            jax.ShapeDtypeStruct((rows, kv_width), BF16),
        ),
        in_specs=[SMEM] + [VMEM] * 2 + [ANY] * 3,
        out_specs=(ANY, VMEM),
        scratch_shapes=late_scratch,
        input_output_aliases={3: 0},
        compiler_params=params(12),
        cost_estimate=cost(2 * rows * width * kv_width, 2 * width * kv_width),
        name="values",
    )(place, normed, whole["v"][1], whole["v"][0], *late["v"])

    query = query.reshape(batches, tok, width)

    def turn_call(turn, left, *operands):
        return pl.pallas_call(
            functools.partial(turn_kernel, turn, sections, chunks, left),
            out_shape=(
                jax.ShapeDtypeStruct((part, width), BF16),
                jax.ShapeDtypeStruct(acc.shape, F32),
                jax.ShapeDtypeStruct(gsum.shape, F32),
                jax.ShapeDtypeStruct(grads.shape, BF16),
                *[jax.ShapeDtypeStruct((kv_rows[b], wide), BF16) for b in left],
            ),
            in_specs=[SMEM] + [VMEM] * 14 + [ANY] + [HBM] * (1 + len(left)),
            out_specs=(VMEM, VMEM, VMEM, HBM) + (HBM,) * len(left),
            scratch_shapes=[
                pltpu.VMEM((part, width), BF16),
                pltpu.VMEM((part, width), F32),
                pltpu.VMEM((part, wide), BF16),
                pltpu.VMEM((GAIN_ROWS, wide), BF16),
                pltpu.SemaphoreType.DMA,
                pltpu.SemaphoreType.DMA((3,)),
            ],
            input_output_aliases={7: 1, 8: 2, 16: 3} | {17 + i: 4 + i for i in range(len(left))},
            compiler_params=params(TURN_MIB),
            cost_estimate=cost(2 * part * width * wide * 8, 2 * width * wide),
        )(*operands)

    gathered = {}
    x_recv = {}
    x_own = x_other = None
    split = sections - 1
    x_turns = exchange_turns(sections, units)
    units_from = 2 * (sections - 1)
    turns = units + units_from
    sent = [recv0, recv0]

    def exchange(value, k, way):
        held = range(split) if way == 0 else range(split, sections)
        size = 2 * lines
        pairs = [
            (s * size + 2 * a + core, s * size + 2 * ((a + k) % lines) + core)
            for s in held
            for a in range(lines)
            for core in range(2)
        ]
        return lax.ppermute(value, ("section", "dp"), pairs)

    def pack():
        own_part, other_part = pl.pallas_call(
            pack_kernel,
            out_shape=(jax.ShapeDtypeStruct((lines, rows, own), BF16),) * 2,
            in_specs=[SMEM] + [VMEM] * (2 * lines - 1),
            out_specs=(VMEM,) * 2,
            compiler_params=params(8),
            cost_estimate=cost(1e8, 4 * lines * rows * own),
            name="pack",
        )(place, x_send[0], *[x_recv[way, k] for way in range(2) for k in range(1, lines)])
        return own_part, swap(other_part)

    for turn in range(turns):
        recv = sent[-2]
        if turn == turns - 1 and batches > 1:
            recv = after(recv, *gathered[batches - 2][:lines])
        left = tuple(b for b in range(batches) if b not in gathered)
        lower, acc, gsum, grads, *updated = turn_call(
            turn,
            left,
            place,
            inv,
            gains,
            key,
            value,
            cosine,
            sine,
            acc,
            gsum,
            cotangent,
            inputs[0],
            query,
            prob,
            key_full,
            value_full,
            recv,
            grads,
            *[kvs[b] for b in left],
        )
        kvs.update(zip(left, updated))
        pairs = [
            (s, s - 1)
            for s in range(1, sections)
            if 0 <= turn - 2 * (sections - 1 - s) < units
        ]
        sent.append(lax.ppermute(lower, "section", pairs) if pairs else recv0)
        for way, at in enumerate(x_turns):
            for k in range(1, lines) if turn == at else ():
                part_k = after(x_send[k], lower)
                x_recv[way, k] = exchange(part_k, k, way)
        for b in range(batches):
            if turn == units_from + (b + 1) * chunks - 1:
                mine = [kvs[b]]
                for k in range(1, lines):
                    mine.append(shifted(kvs[b], k))
                gathered[b] = mine + [swap(m) for m in mine]

    x_own, x_other = pack()
    flops = 2 * 2 * lines * tok * own * wide
    final = batches - 1
    operands = [kv for b in range(final) for kv in gathered[b]] + gathered[final][:lines]
    partial = pl.pallas_call(
        functools.partial(weight_kernel, tok, lines, batches),
        out_shape=jax.ShapeDtypeStruct((own, wide), F32),
        in_specs=[VMEM] * (2 + len(operands)),
        out_specs=VMEM,
        compiler_params=params(24),
        cost_estimate=cost(flops, 4 * own * wide),
        name="weights",
    )(x_own, x_other, *operands)
    key_grad, value_grad, gain_grad = pl.pallas_call(
        functools.partial(weight_last_kernel, tok, lines, batches),
        out_shape=(
            jax.ShapeDtypeStruct((own, kv_width), F32),
            jax.ShapeDtypeStruct((own, kv_width), F32),
            jax.ShapeDtypeStruct((1, own), F32),
        ),
        in_specs=[SMEM] + [VMEM] * (2 + 2 * lines),
        out_specs=(VMEM,) * 3,
        compiler_params=params(24),
        cost_estimate=cost(flops, 4 * own * wide),
        name="weights_last",
    )(place, x_other, partial, *gathered[final])
    return (grads[None], key_grad[None], value_grad[None], gain_grad)


def exchange_turns(sections, units):
    end = 2 * (sections - 1) + units - 2
    return min(1, end), min(units + 1, end)


def solution(mesh):
    in_specs = (
        P("section", None, "dp", None),
        P(None, "dp", None),
        P("section", "dp"),
        P("section", "dp", None),
        P("section", "dp", None),
        P("section", None),
    )
    out_specs = (
        P("section", None, "dp", None),
        P("section", "dp", None),
        P("section", "dp", None),
        P("section", "dp"),
    )

    return jax.shard_map(body, mesh=mesh, in_specs=in_specs, out_specs=out_specs, check_vma=False)
```
